32 devices in a mesh: comm: 4 (over z), arc: 8 (over y, x, core).
Axes of the slice: x: 2, y: 2, z: 4, core: 2. Of those that a mesh axis runs over, the one named last changes fastest.
Arguments:
- prev_dist: float32 [512, 2048], P('comm', 'arc'), may hold values from 0 to 4
- source_node: int32 [512], P('comm'), may hold values from 0 to 2047, as said below
- arc_tail: int32 [16, 2048], P(None, 'arc'), may hold values from 0 to 2047, as said below
- base_cost: float32 [16, 2048], P(None, 'arc'), may hold values from 0.05 to 1
- arc_price: float32 [16, 2048], P(None, 'arc'), may hold values from 0 to 1
- capacity: float32 [16, 2048], P(None, 'arc')
- path_arcs: int32 [512, 128], P(('comm', 'arc')), may hold values from 0 to 32767, as said below
- demand: float32 [512], P(('comm', 'arc')), may hold values from 0.5 to 2
Outputs:
- final_dist: float32 [512, 2048], P('comm', 'arc')
- new_price: float32 [16, 2048], P(None, 'arc')
The draws below stay inside these ranges and needn't reach their ends.
Inputs may be any that keep to these rules, and one draw needn't show every extreme that they name: `arc_tail`: the tail of arc s * 2048 + v lies in a node block (nodes 128 b to 128 b + 127) at most 2 blocks before or after v's block, counted around the cycle of blocks. Row k is a walk: the head of path_arcs[k, h + 1] (its id modulo 2048) is the tail of path_arcs[k, h]. `source_node`: the tail of path_arcs[k, 127].
All inputs are finite; a program needn't handle non-finite values.
Results may differ from the reference program's by a relative error of at most 0.00002.
Values sent between devices are 32-bit elements; how exact they have to be, the bound alone decides.
A program may use at most 64 MiB of HBM per device.

```python
import math
import jax
import jax.numpy as jnp
from jax import lax

LANES = 128
BLK_DEV = 2
IN_DEG = 16
SWEEPS = 8
HOPS = 128
NODES = 2048
K = 512


def make_tails(key):
    tail_key = jax.random.fold_in(key, 11)
    key_pair = jax.random.split(tail_key, 2)
    head_nodes = jnp.arange(NODES, dtype=jnp.int32)
    head_block = head_nodes // LANES
    blocks_all = NODES // LANES
    offset = jax.random.randint(key_pair[0], (IN_DEG, NODES), -BLK_DEV, BLK_DEV + 1)
    lane_pick = jax.random.randint(key_pair[1], (IN_DEG, NODES), 0, LANES)
    return (jnp.mod(head_block[None, :] + offset, blocks_all) * LANES + lane_pick).astype(jnp.int32)


def make_walks(key):
    tail_nodes = make_tails(key).reshape(-1)
    walk_key = jax.random.fold_in(key, 23)
    key_pair = jax.random.split(walk_key, 2)
    sink_nodes = jax.random.randint(key_pair[0], (K,), 0, NODES).astype(jnp.int32)
    slot_picks = jax.random.randint(key_pair[1], (HOPS, K), 0, IN_DEG).astype(jnp.int32)

    def advance(current, picked):
        arc_ids = picked * NODES + current
        return (tail_nodes[arc_ids], arc_ids)
    endpoint, walked = lax.scan(advance, sink_nodes, slot_picks)
    return (walked.T.astype(jnp.int32), endpoint.astype(jnp.int32))


def draw_arc_tail(key, part):
    return make_tails(key)


def draw_path_arcs(key, part):
    return make_walks(key)[0]


def draw_source_node(key, part):
    return make_walks(key)[1]


def draw_capacity(key, part):
    mean_load = K * HOPS / (IN_DEG * NODES)
    positions = jnp.arange(NODES, dtype=jnp.float32) / NODES
    rough_factor = jnp.exp(jax.random.uniform(key, (IN_DEG, NODES), jnp.float32, math.log(0.3), math.log(3.0)))
    return (mean_load * rough_factor * (0.5 + 1.5 * positions)[None, :]).astype(jnp.float32)


def block_scale(own_key, dims, pieces, least, largest):
    loudness = 1.0
    for dim, parts in pieces:
        heights = jax.random.uniform(jax.random.fold_in(jax.random.fold_in(own_key, 6), dim), (parts,), jnp.float32, least / len(pieces), largest / len(pieces))
        loudness = loudness * jnp.repeat(jnp.exp(heights), dims[dim] // parts).reshape((-1,) + (1,) * (len(dims) - 1 - dim))
    return loudness


def setup_inputs(seed: int = 0) -> dict:
    key_of = jax.random.split(jax.random.key(seed), 9)
    return {
        "prev_dist": jnp.clip(4.0 * jax.random.uniform(key_of[0], (K, NODES), jnp.float32) ** block_scale(key_of[0], (K, NODES), ((0, 4), (1, 8)), -0.2, 0.2), 0.0, 4.0),
        "source_node": draw_source_node(jax.random.fold_in(key_of[8], 71), 0),
        "arc_tail": draw_arc_tail(jax.random.fold_in(key_of[8], 71), 0),
        "base_cost": jnp.clip(jnp.exp(math.log(1.0) - 2.9957323 * jax.random.uniform(key_of[3], (IN_DEG, NODES), jnp.float32) ** block_scale(key_of[3], (IN_DEG, NODES), ((1, 8),), -0.2, 0.2)), 0.05, 1.0),
        "arc_price": jnp.clip(1.0 * jax.random.uniform(key_of[4], (IN_DEG, NODES), jnp.float32) ** block_scale(key_of[4], (IN_DEG, NODES), ((1, 8),), -0.2, 0.2), 0.0, 1.0),
        "capacity": draw_capacity(jax.random.fold_in(key_of[8], 71), 0),
        "path_arcs": draw_path_arcs(jax.random.fold_in(key_of[8], 71), 0),
        "demand": jnp.clip(jnp.exp(math.log(2.0) - 1.3862944 * jax.random.uniform(key_of[7], (K,), jnp.float32) ** block_scale(key_of[7], (K,), ((0, 32),), -0.2, 0.2)), 0.5, 2.0),
    }


step_size = 0.25
eps_value = 1e-06

def reference(prev_dist, source_node, arc_tail, base_cost, arc_price, capacity, path_arcs, demand):
    arc_weight = base_cost + arc_price
    node_ids = jnp.arange(NODES, dtype=jnp.int32)
    distance = jnp.where(node_ids[None, :] == source_node[:, None], jnp.float32(0.0), prev_dist)
    for sweep_number in range(SWEEPS):
        best_dist = distance
        for in_slot in range(IN_DEG):
            candidate = jnp.take(distance, arc_tail[in_slot], axis=1) + arc_weight[in_slot][None, :]
            best_dist = jnp.minimum(best_dist, candidate)
        distance = best_dist
    amounts = jnp.broadcast_to(demand[:, None], path_arcs.shape).reshape(-1)
    flattened = jnp.zeros((IN_DEG * NODES,), jnp.float32).at[path_arcs.reshape(-1)].add(amounts)
    arc_flow = flattened.reshape(IN_DEG, NODES)
    gradient = arc_flow - capacity
    scale_root = jnp.sqrt(jnp.sum(gradient * gradient) / (IN_DEG * NODES) + eps_value)
    new_price = jnp.maximum(arc_price + step_size * gradient / scale_root, jnp.float32(0.0))
    return (distance, new_price)
```

```python
import functools

import jax
import jax.numpy as jnp
from jax import lax
from jax.experimental import pallas as pl
from jax.experimental.pallas import tpu as pltpu
from jax.sharding import PartitionSpec as P

SWEEPS = 8
LANES = 128
REACH = 2
OFFS = 2 * REACH + 1
PAD = 8
FIXED = 8
BUCKETS = (3, 6, 9, 12, 18)

step_size = 0.25
eps_value = 1e-06
MESH_ID = pl.DeviceIdType.MESH


def send(src, dst, ss, rs, dev):
    return pltpu.make_async_remote_copy(src_ref=src, dst_ref=dst, send_sem=ss, recv_sem=rs,
                                        device_id=dev, device_id_type=MESH_ID)


def flip(index, bits, size):
    return sum(lax.rem(index // b + (bits // b) % 2, 2) * b for b in (1 << n for n in range((size - 1).bit_length())))


def others(A, me):
    chips = A // 2
    assert chips & (chips - 1) == 0
    far = sorted(range(1, chips), key=lambda bits: -bits.bit_count())
    core = lax.rem(me, 2)
    out = [2 * flip(me // 2, bits, chips) + lax.rem(core + c, 2) for bits in far for c in (0, 1)]
    return out + [2 * (me // 2) + 1 - core]


def greet(A, C, me, mc, along_comm):
    barrier = pltpu.get_barrier_semaphore()
    for i in range(1, A):
        pl.semaphore_signal(barrier, inc=1, device_id=(mc, lax.rem(me + i, A)), device_id_type=MESH_ID)
    for i in range(1, C if along_comm else 1):
        pl.semaphore_signal(barrier, inc=1, device_id=(lax.rem(mc + i, C), me), device_id_type=MESH_ID)
    return lambda: pl.semaphore_wait(barrier, A - 1 + (C - 1 if along_comm else 0))


def gather_kernel(A, C, m,
                  source_ref, demand_ref, dist_hbm, tail_hbm, cost_hbm, price_hbm, cap_hbm, path_hbm,
                  X0, KT, WW, COUNT, PI, PW, grad_ref, price_ref,
                  D, dist_ref, tail_ref, cost_ref, cap_ref, path_ref,
                  T, W, F, RF, G,
                  in_s, d_s, d_r, t_s, t_r, w_s, w_r, f_s, f_r, g_s, g_r):
    degree, span = tail_ref.shape
    NB = A * m
    chips = A // 2
    node_count = NB * LANES
    groups = NB // 8
    me = lax.axis_index("arc")
    mc = lax.axis_index("comm")
    chip, core = me // 2, lax.rem(me, 2)
    twin = 2 * chip + 1 - core
    block_lanes = [slice(h * LANES, (h + 1) * LANES) for h in range(m)]

    pairs = ((path_hbm, path_ref), (tail_hbm, tail_ref), (cost_hbm, cost_ref), (price_hbm, price_ref),
             (dist_hbm, dist_ref), (cap_hbm, cap_ref))
    loads = [pltpu.make_async_copy(src, dst, in_s.at[i]) for i, (src, dst) in enumerate(pairs)]
    for c in loads:
        c.start()
    wait_peers = greet(A, C, me, mc, True)
    loads[0].wait()

    total_rows = NB * degree
    shift_nodes = (node_count - 1).bit_length()
    assert 1 << shift_nodes == node_count
    path = path_ref[...]
    slot_of = path >> shift_nodes
    node_of = path & (node_count - 1)
    row_of = (node_of >> 7) * degree + slot_of
    lane_of = node_of & (LANES - 1)
    row_iota = lax.broadcasted_iota(jnp.int32, (total_rows, LANES), 0)
    lane_iota = lax.broadcasted_iota(jnp.int32, (LANES, LANES), 0)
    acc = jnp.zeros((total_rows, LANES), jnp.float32)
    for k in range(path.shape[0]):
        hi = jnp.where(row_iota == row_of[k:k + 1, :], 1.0, 0.0).astype(jnp.bfloat16)
        lo = jnp.where(lane_iota == lane_of[k:k + 1, :], 1.0, 0.0).astype(jnp.bfloat16)
        count = lax.dot_general(hi, lo, (((1,), (1,)), ((), ())), preferred_element_type=jnp.float32)
        acc = acc + count * demand_ref[k]
    F[...] = acc.reshape(F.shape)

    for c in loads[1:]:
        c.wait()
    for h in range(m):
        W[me * m + h] = cost_ref[:, block_lanes[h]] + price_ref[:, block_lanes[h]]
        T[me * m + h] = tail_ref[:, block_lanes[h]]
        D[me * m + h] = dist_ref[me, :, block_lanes[h]]
    wait_peers()

    def share(owner, n, dev):
        at = pl.ds(owner * m, m)
        return [send(T.at[at], T.at[at], t_s.at[n], t_r.at[n], dev),
                send(W.at[at], W.at[at], w_s.at[n], w_r.at[n], dev)]

    flows, dists = [], []
    for i, j in enumerate(others(A, me), 1):
        flows.append(send(F.at[j], RF.at[me], f_s.at[i - 1], f_r.at[i - 1], (mc, j)))
        for h in range(m):
            n = (i - 1) * m + h
            dists.append(send(dist_ref.at[j, :, block_lanes[h]], D.at[me * m + h], d_s.at[n], d_r.at[n], (mc, j)))
    far = []
    for i in range(1, chips):
        far += share(me, i - 1, (mc, 2 * flip(chip, i, chips) + core))
    near = share(me, chips - 1, (mc, twin))
    for c in flows + far + near + dists:
        c.start()
    passed = []
    for i in range(1, chips):
        for c in far[2 * (i - 1):2 * i]:
            c.wait()
        owner = 2 * flip(chip, i, chips) + core
        onward = share(owner, chips - 1 + i, (mc, twin))
        for c in onward:
            c.start()
        passed += onward

    for c in flows:
        c.wait()
    total = F[me]
    for i in range(1, A):
        total = total + RF[lax.rem(me + i, A)]
    G[mc] = total
    shares = [send(G.at[mc], G.at[mc], g_s.at[i - 1], g_r.at[i - 1], (lax.rem(mc + i, C), me)) for i in range(1, C)]
    for c in shares:
        c.start()
    for c in near + passed:
        c.wait()

    sub = lax.broadcasted_iota(jnp.int32, (8, LANES), 0)
    for g in range(groups):
        count = [jnp.zeros((8, LANES), jnp.int32)] * OFFS
        for s in range(degree):
            tail = T[8 * g:8 * g + 8, s, :]
            rel = (tail >> 7) - (8 * g + sub) + REACH
            rel = jnp.where(rel < 0, rel + NB, rel)
            rel = jnp.where(rel >= NB, rel - NB, rel)
            rank = count[0]
            for o in range(1, OFFS):
                rank = jnp.where(rel == o, count[o], rank)
            count = [c + jnp.where(rel == o, 1, 0) for o, c in enumerate(count)]
            KT[g, s] = ((rel * degree + rank) << 7) + (tail & (LANES - 1))
            WW[g, s] = W[8 * g:8 * g + 8, s, :]
        for o in range(OFFS):
            COUNT[g, o] = count[o]

    def build(p, _):
        key = lax.div(p, FIXED) * degree + lax.rem(p, FIXED)
        for g in range(groups):
            PI[g, p], PW[g, p] = arc_of(KT, WW, g, key, degree)
        return 0

    lax.fori_loop(0, OFFS * FIXED, build, 0)

    for c in dists:
        c.wait()
    lane = lax.broadcasted_iota(jnp.int32, (8, LANES), 1)
    for g in range(groups):
        node = (8 * g + sub) * LANES + lane
        for k in range(D.shape[1]):
            old = D[8 * g:8 * g + 8, k, :]
            put(X0.at[k], g, groups, jnp.where(node == source_ref[me * D.shape[1] + k], 0.0, old))
    for c in shares:
        c.wait()
    flow = G[0]
    for i in range(1, C):
        flow = flow + G[i]
    for h in range(m):
        grad_ref[h * degree:(h + 1) * degree, :] = flow[h * degree:(h + 1) * degree, :] - cap_ref[:, block_lanes[h]]


def arc_of(KT, WW, g, key, degree):
    kept = jnp.zeros((8, LANES), jnp.int32)
    weight = jnp.full((8, LANES), jnp.inf, jnp.float32)
    for s in range(degree):
        kt = KT[g, s]
        hit = (kt >> 7) == key
        kept = jnp.where(hit, kt, kept)
        weight = jnp.where(hit, WW[g, s], weight)
    return kept & (LANES - 1), weight


def put(row, g, groups, value):
    row[PAD + 8 * g:PAD + 8 * g + 8, :] = value
    if g == 0:
        row[PAD + 8 * groups:PAD + 8 * groups + REACH, :] = value[:REACH]
    if g == groups - 1:
        row[PAD - REACH:PAD, :] = value[8 - REACH:]


def sweep_kernel(X0, KT, WW, COUNT, PI, PW, Y, X, EI, EW, OFF):
    rows = X0.shape[0]
    groups, degree = KT.shape[:2]

    counts = [[jnp.max(COUNT[g, o]) for o in range(OFFS)] for g in range(groups)]
    for g in range(groups):
        for k in range(rows):
            put(X.at[0, k], g, groups, X0[k, PAD + 8 * g:PAD + 8 * g + 8, :])

    ends = []
    for g in range(groups):
        pos = 0
        for o in range(OFFS):
            def build(i, pos, g=g, o=o):
                EI[g, pos], EW[g, pos] = arc_of(KT, WW, g, o * degree + i, degree)
                OFF[g, pos] = o
                return pos + 1
            pos = lax.fori_loop(FIXED, counts[g][o], build, pos)
        ends.append(pos)
    most = functools.reduce(jnp.maximum, ends)
    sizes = BUCKETS + (OFFS * (degree - FIXED),)
    room = sizes[-1]
    for size in reversed(sizes[:-1]):
        room = jnp.where(most <= size, size, room)

    for g in range(groups):
        def fill(p, _, g=g):
            EI[g, p] = jnp.zeros((8, LANES), jnp.int32)
            EW[g, p] = jnp.full((8, LANES), jnp.inf, jnp.float32)
            OFF[g, p] = 0
            return 0
        lax.fori_loop(ends[g], room, fill, 0)

    def sweep(extra, t):
        read = lax.rem(t, 2)
        for g in range(groups):
            base = PAD + 8 * g - REACH
            best = [X[read, k, PAD + 8 * g:PAD + 8 * g + 8, :] for k in range(rows)]
            todo = [(o + base, PI, PW, o * FIXED + i) for o in range(OFFS) for i in range(FIXED)]
            todo += [(OFF[g, p] + base, EI, EW, p) for p in range(extra)]
            for start, index, weight, p in todo:
                idx = index[g, p]
                w = weight[g, p]
                for k in range(rows):
                    got = jnp.take_along_axis(X[read, k, pl.ds(start, 8), :], idx, axis=1,
                                              mode="promise_in_bounds")
                    best[k] = jnp.minimum(best[k], got + w)
            for k in range(rows):
                put(X.at[1 - read, k], g, groups, best[k])

    for extra in sizes:
        @pl.when(room == extra)
        def _(extra=extra):
            def one(t, _):
                sweep(extra, t)
                return 0
            lax.fori_loop(0, SWEEPS, one, 0)

    for g in range(groups):
        for k in range(rows):
            Y[8 * g:8 * g + 8, k, :] = X[SWEEPS % 2, k, PAD + 8 * g:PAD + 8 * g + 8, :]


def finish_kernel(A, C, m,
                  Y, grad_ref, price_ref,
                  out_ref, newp_ref,
                  Q, o_s, o_r, q_s, q_r):
    degree, span = price_ref.shape
    node_count = A * m * LANES
    me = lax.axis_index("arc")
    mc = lax.axis_index("comm")
    block_lanes = [slice(h * LANES, (h + 1) * LANES) for h in range(m)]

    wait_peers = greet(A, C, me, mc, False)
    gradient = [grad_ref[h * degree:(h + 1) * degree, :] for h in range(m)]
    Q[me] = sum(g * g for g in gradient)
    for h in range(m):
        out_ref[me, :, block_lanes[h]] = Y[me * m + h]
    wait_peers()
    norms, outs = [], []
    for i, j in enumerate(others(A, me), 1):
        norms.append(send(Q.at[me], Q.at[me], q_s.at[i - 1], q_r.at[i - 1], (mc, j)))
        for h in range(m):
            n = (i - 1) * m + h
            outs.append(send(Y.at[j * m + h], out_ref.at[me, :, block_lanes[h]], o_s.at[n], o_r.at[n], (mc, j)))
    for c in norms + outs:
        c.start()
    for c in norms:
        c.wait()
    square = Q[0]
    for i in range(1, A):
        square = square + Q[i]
    scale_root = jnp.sqrt(jnp.sum(square) / (degree * node_count) + eps_value)
    for h in range(m):
        newp_ref[:, block_lanes[h]] = jnp.maximum(
            price_ref[:, block_lanes[h]] + step_size * gradient[h] / scale_root, 0.0)
    for c in outs:
        c.wait()


def store_kernel(out_ref, newp_ref, out_hbm, newp_hbm, sem):
    copies = [pltpu.make_async_copy(out_ref, out_hbm, sem.at[0]), pltpu.make_async_copy(newp_ref, newp_hbm, sem.at[1])]
    for c in copies:
        c.start()
    for c in copies:
        c.wait()


def shards(A, C, prev_dist, source_node, arc_tail, base_cost, arc_price, capacity, path_arcs, demand):
    commodities, span = prev_dist.shape
    degree = arc_tail.shape[0]
    rows = commodities // A
    m = span // LANES
    NB = A * m
    assert NB % 8 == 0 and degree >= FIXED
    f32, i32 = jnp.float32, jnp.int32
    groups = NB // 8
    extras = OFFS * (degree - FIXED)
    vmem = pl.BlockSpec(memory_space=pltpu.VMEM)
    smem = pl.BlockSpec(memory_space=pltpu.SMEM)
    hbm = pl.BlockSpec(memory_space=pltpu.HBM)
    sems = pltpu.SemaphoreType.DMA
    kept_words = (rows * (NB + 2 * PAD) + 16 * groups * degree + 8 * groups * OFFS * (1 + 2 * FIXED)) * LANES
    limit = 64_600_000 - 4 * kept_words
    X0, KT, WW, COUNT, PI, PW, gradient, price = pl.pallas_call(
        functools.partial(gather_kernel, A, C, m),
        out_shape=(pltpu.VMEM((rows, NB + 2 * PAD, LANES), f32), pltpu.VMEM((groups, degree, 8, LANES), i32),
                   pltpu.VMEM((groups, degree, 8, LANES), f32), pltpu.VMEM((groups, OFFS, 8, LANES), i32),
                   pltpu.VMEM((groups, OFFS * FIXED, 8, LANES), i32),
                   pltpu.VMEM((groups, OFFS * FIXED, 8, LANES), f32), pltpu.VMEM((m * degree, LANES), f32),
                   pltpu.VMEM((degree, span), f32)),
        in_specs=[smem] * 2 + [hbm] * 6,
        out_specs=(vmem,) * 8,
        scratch_shapes=[
            pltpu.VMEM((NB, rows, LANES), f32),
            pltpu.VMEM((A, rows, span), f32),
            pltpu.VMEM((degree, span), i32),
            pltpu.VMEM((degree, span), f32),
            pltpu.VMEM((degree, span), f32),
            pltpu.VMEM(path_arcs.shape, i32),
            pltpu.VMEM((NB, degree, LANES), i32),
            pltpu.VMEM((NB, degree, LANES), f32),
            pltpu.VMEM((A, m * degree, LANES), f32),
            pltpu.VMEM((A, m * degree, LANES), f32),
            pltpu.VMEM((C, m * degree, LANES), f32),
        ] + [sems((6,))] + [sems(((A - 1) * m,))] * 2 + [sems((A - 1,))] * 6 + [sems((C - 1,))] * 2,
        compiler_params=pltpu.CompilerParams(collective_id=0, has_side_effects=True, vmem_limit_bytes=limit),
    )(source_node, demand, prev_dist.reshape(A, rows, span), arc_tail, base_cost, arc_price, capacity, path_arcs)
    Y = pl.pallas_call(
        sweep_kernel,
        out_shape=pltpu.VMEM((NB, rows, LANES), f32),
        in_specs=[vmem] * 6,
        out_specs=vmem,
        scratch_shapes=[
            pltpu.VMEM((2, rows, NB + 2 * PAD, LANES), f32),
            pltpu.VMEM((groups, extras, 8, LANES), i32),
            pltpu.VMEM((groups, extras, 8, LANES), f32),
            pltpu.SMEM((groups, extras), i32),
        ],
        compiler_params=pltpu.CompilerParams(vmem_limit_bytes=24 * 2**20),
    )(X0, KT, WW, COUNT, PI, PW)
    out, new_price = pl.pallas_call(
        functools.partial(finish_kernel, A, C, m),
        out_shape=(pltpu.VMEM((A, rows, span), f32), pltpu.VMEM((degree, span), f32)),
        in_specs=[vmem] * 3,
        out_specs=(vmem, vmem),
        scratch_shapes=[pltpu.VMEM((A, degree, LANES), f32)] + [sems(((A - 1) * m,))] * 2 + [sems((A - 1,))] * 2,
        compiler_params=pltpu.CompilerParams(collective_id=1, has_side_effects=True, vmem_limit_bytes=24 * 2**20),
    )(Y, gradient, price)
    out, new_price = pl.pallas_call(
        store_kernel,
        out_shape=(jax.ShapeDtypeStruct(out.shape, f32), jax.ShapeDtypeStruct(new_price.shape, f32)),
        in_specs=[vmem] * 2,
        out_specs=(hbm, hbm),
        scratch_shapes=[sems((2,))],
        compiler_params=pltpu.CompilerParams(vmem_limit_bytes=24 * 2**20),
    )(out, new_price)
    return (out.reshape(commodities, span), new_price)


def solution(mesh):
    in_specs = (
        P("comm", "arc"),
        P("comm"),
        P(None, "arc"),
        P(None, "arc"),
        P(None, "arc"),
        P(None, "arc"),
        P(("comm", "arc"), None),
        P(("comm", "arc")),
    )
    out_specs = (P("comm", "arc"), P(None, "arc"))
    body = functools.partial(shards, mesh.shape["arc"], mesh.shape["comm"])
    return jax.shard_map(body, mesh=mesh, in_specs=in_specs, out_specs=out_specs, check_vma=False)
```

```python
import functools

import jax
import jax.numpy as jnp
from jax import lax
from jax.experimental import pallas as pl
from jax.experimental.pallas import tpu as pltpu
from jax.sharding import PartitionSpec as P

SWEEPS = 8
LANES = 128
REACH = 2
OFFS = 2 * REACH + 1
PAD = 8
FIXED = 7
BUCKETS = (2, 5)
CHUNK = 5
MEET = 2
HALF = LANES // 2

step_size = 0.25
eps_value = 1e-06
MESH_ID = pl.DeviceIdType.MESH


def send(src, dst, ss, rs, dev):
    return pltpu.make_async_remote_copy(src_ref=src, dst_ref=dst, send_sem=ss, recv_sem=rs,
                                        device_id=dev, device_id_type=MESH_ID)


def flip(index, bits, size):
    return sum(lax.rem(index // b + (bits // b) % 2, 2) * b for b in (1 << n for n in range((size - 1).bit_length())))


def others(A, me):
    chips = A // 2
    assert chips & (chips - 1) == 0
    far = sorted(range(1, chips), key=lambda bits: -bits.bit_count())
    core = lax.rem(me, 2)
    out = [2 * flip(me // 2, bits, chips) + lax.rem(core + c, 2) for bits in far for c in (0, 1)]
    return out + [2 * (me // 2) + 1 - core]


def greet(A, C, me, mc, along_comm):
    barrier = pltpu.get_barrier_semaphore()
    for i in range(1, A):
        pl.semaphore_signal(barrier, inc=1, device_id=(mc, lax.rem(me + i, A)), device_id_type=MESH_ID)
    for i in range(1, C if along_comm else 1):
        pl.semaphore_signal(barrier, inc=1, device_id=(lax.rem(mc + i, C), me), device_id_type=MESH_ID)
    return lambda: pl.semaphore_wait(barrier, A - 1 + (C - 1 if along_comm else 0))


def gather_kernel(A, C, m,
                  source_ref, demand_ref, dist_hbm, tail_hbm, cost_hbm, price_hbm, cap_hbm, path_hbm,
                  X0, KT, WW, COUNT, CAP, PI, PW, PV, flow_ref, price_ref, cap_ref,
                  D, dist_ref, tail_ref, cost_ref, path_ref,
                  T, W, F, RF,
                  in_s, d_s, d_r, t_s, t_r, w_s, w_r, f_s, f_r):
    degree, span = tail_ref.shape
    NB = A * m
    chips = A // 2
    node_count = NB * LANES
    groups = NB // 8
    me = lax.axis_index("arc")
    mc = lax.axis_index("comm")
    chip, core = me // 2, lax.rem(me, 2)
    twin = 2 * chip + 1 - core
    block_lanes = [slice(h * LANES, (h + 1) * LANES) for h in range(m)]

    pairs = ((path_hbm, path_ref), (tail_hbm, tail_ref), (cost_hbm, cost_ref), (price_hbm, price_ref),
             (dist_hbm, dist_ref), (cap_hbm, cap_ref))
    loads = [pltpu.make_async_copy(src, dst, in_s.at[i]) for i, (src, dst) in enumerate(pairs)]
    for c in loads:
        c.start()
    wait_peers = greet(A, C, me, mc, False)
    loads[0].wait()

    total_rows = NB * degree
    shift_nodes = (node_count - 1).bit_length()
    assert 1 << shift_nodes == node_count
    path = path_ref[...]
    slot_of = path >> shift_nodes
    node_of = path & (node_count - 1)
    row_of = (node_of >> 7) * degree + slot_of
    lane_of = node_of & (LANES - 1)
    row_iota = lax.broadcasted_iota(jnp.int32, (total_rows, LANES), 0)
    lane_iota = lax.broadcasted_iota(jnp.int32, (LANES, LANES), 0)
    acc = jnp.zeros((total_rows, LANES), jnp.float32)
    for k in range(path.shape[0]):
        hi = jnp.where(row_iota == row_of[k:k + 1, :], 1.0, 0.0).astype(jnp.bfloat16)
        lo = jnp.where(lane_iota == lane_of[k:k + 1, :], 1.0, 0.0).astype(jnp.bfloat16)
        count = lax.dot_general(hi, lo, (((1,), (1,)), ((), ())), preferred_element_type=jnp.float32)
        acc = acc + count * demand_ref[k]
    F[...] = acc.reshape(F.shape)

    for c in loads[1:]:
        c.wait()
    for h in range(m):
        W[me * m + h] = cost_ref[:, block_lanes[h]] + price_ref[:, block_lanes[h]]
        T[me * m + h] = tail_ref[:, block_lanes[h]]
        D[me * m + h] = dist_ref[me, :, block_lanes[h]]
    wait_peers()

    def share(owner, n, dev):
        at = pl.ds(owner * m, m)
        return [send(T.at[at], T.at[at], t_s.at[n], t_r.at[n], dev),
                send(W.at[at], W.at[at], w_s.at[n], w_r.at[n], dev)]

    flows, dists = [], []
    for i, j in enumerate(others(A, me), 1):
        flows.append(send(F.at[j], RF.at[me], f_s.at[i - 1], f_r.at[i - 1], (mc, j)))
        for h in range(m):
            n = (i - 1) * m + h
            dists.append(send(dist_ref.at[j, :, block_lanes[h]], D.at[me * m + h], d_s.at[n], d_r.at[n], (mc, j)))
    far = []
    for i in range(1, chips):
        far += share(me, i - 1, (mc, 2 * flip(chip, i, chips) + core))
    near = share(me, chips - 1, (mc, twin))
    for c in flows + far + near + dists:
        c.start()
    passed = []
    for i in range(1, chips):
        for c in far[2 * (i - 1):2 * i]:
            c.wait()
        owner = 2 * flip(chip, i, chips) + core
        onward = share(owner, chips - 1 + i, (mc, twin))
        for c in onward:
            c.start()
        passed += onward

    for c in near + passed:
        c.wait()

    sub = lax.broadcasted_iota(jnp.int32, (8, LANES), 0)
    for g in range(groups):
        count = [jnp.zeros((8, LANES), jnp.int32)] * OFFS
        for s in range(degree):
            tail = T[8 * g:8 * g + 8, s, :]
            rel = (tail >> 7) - (8 * g + sub) + REACH
            rel = jnp.where(rel < 0, rel + NB, rel)
            rel = jnp.where(rel >= NB, rel - NB, rel)
            rank = count[0]
            for o in range(1, OFFS):
                rank = jnp.where(rel == o, count[o], rank)
            count = [c + jnp.where(rel == o, 1, 0) for o, c in enumerate(count)]
            KT[g, s] = ((rel * degree + rank) << 7) + (tail & (LANES - 1))
            WW[g, s] = W[8 * g:8 * g + 8, s, :]
        for o in range(OFFS):
            free = FIXED - jnp.minimum(pltpu.roll(count[o], HALF, 1), FIXED)
            CAP[g, o] = FIXED + free
            COUNT[g, o] = jnp.maximum(count[o] - FIXED - free, 0)

    def build(o, _):
        for g in range(groups):
            kts = [KT[g, s] for s in range(degree)]
            ranks = [(kt >> 7) - o * degree for kt in kts]
            weights = [WW[g, s] for s in range(degree)]

            def find(rank):
                kept = jnp.zeros((8, LANES), jnp.int32)
                weight = jnp.full((8, LANES), jnp.inf, jnp.float32)
                for s in range(rank, degree):
                    hit = ranks[s] == rank
                    kept = jnp.where(hit, kts[s], kept)
                    weight = jnp.where(hit, weights[s], weight)
                return kept, weight

            for i in range(FIXED):
                own_kept, own_weight = find(i)
                far_kept, far_weight = [pltpu.roll(x, HALF, 1) for x in find(2 * FIXED - 1 - i)]
                mine = own_weight < jnp.inf
                p = o * FIXED + i
                PI[g, p] = jnp.where(mine, own_kept, far_kept) & (LANES - 1)
                PW[g, p] = own_weight
                PV[g, p] = jnp.where(mine, jnp.inf, far_weight)
        return 0

    lax.fori_loop(0, OFFS, build, 0)

    for c in dists:
        c.wait()
    lane = lax.broadcasted_iota(jnp.int32, (8, LANES), 1)
    for g in range(groups):
        node = (8 * g + sub) * LANES + lane
        for k in range(D.shape[1]):
            old = D[8 * g:8 * g + 8, k, :]
            put(X0.at[k], g, groups, jnp.where(node == source_ref[me * D.shape[1] + k], 0.0, old))
    for c in flows:
        c.wait()
    total = F[me]
    for i in range(1, A):
        total = total + RF[lax.rem(me + i, A)]
    flow_ref[...] = total


def arc_of(KT, WW, g, key, degree):
    kept = jnp.zeros((8, LANES), jnp.int32)
    weight = jnp.full((8, LANES), jnp.inf, jnp.float32)
    for s in range(degree):
        kt = KT[g, s]
        hit = (kt >> 7) == key
        kept = jnp.where(hit, kt, kept)
        weight = jnp.where(hit, WW[g, s], weight)
    return kept & (LANES - 1), weight


def put(row, g, groups, value):
    row[PAD + 8 * g:PAD + 8 * g + 8, :] = value
    if g == 0:
        row[PAD + 8 * groups:PAD + 8 * groups + REACH, :] = value[:REACH]
    if g == groups - 1:
        row[PAD - REACH:PAD, :] = value[8 - REACH:]


def list_kernel(KT, WW, COUNT, CAP, EI, EW, OFF, choice):
    groups, degree = KT.shape[:2]
    counts = [[jnp.max(COUNT[g, o]) for o in range(OFFS)] for g in range(groups)]
    ends = []
    for g in range(groups):
        pos = 0
        for o in range(OFFS):
            def build(i, pos, g=g, o=o):
                rank = CAP[g, o] + i
                key = jnp.where(rank < degree, o * degree + rank, -1)
                EI[g, pos], EW[g, pos] = arc_of(KT, WW, g, key, degree)
                OFF[g, pos] = o
                return pos + 1
            pos = lax.fori_loop(0, counts[g][o], build, pos)
        ends.append(pos)
    most = functools.reduce(jnp.maximum, ends)
    room = EI.shape[1]
    which = len(BUCKETS)
    for n, size in reversed(list(enumerate(BUCKETS))):
        room = jnp.where(most <= size, size, room)
        which = jnp.where(most <= size, n, which)
    choice[0] = which

    for g in range(groups):
        def fill(p, _, g=g):
            EI[g, p] = jnp.zeros((8, LANES), jnp.int32)
            EW[g, p] = jnp.full((8, LANES), jnp.inf, jnp.float32)
            OFF[g, p] = 0
            return 0
        lax.fori_loop(ends[g], room, fill, 0)


def sweep_kernel(A, C, m, extra,
                 OFF, X0, PI, PW, PV, EI, EW, flow_ref, price_ref, cap_ref,
                 out_ref, newp_ref,
                 X, Y, G, Q,
                 g_s, g_r, q_s, q_r, o_s, o_r):
    rows = X0.shape[0]
    groups = PI.shape[0]
    degree, span = price_ref.shape
    node_count = A * m * LANES
    me = lax.axis_index("arc")
    mc = lax.axis_index("comm")
    block_lanes = [slice(h * LANES, (h + 1) * LANES) for h in range(m)]

    wait_peers = greet(A, C, me, mc, True)
    G[mc] = flow_ref[...]
    for g in range(groups):
        for k in range(rows):
            put(X.at[0, k], g, groups, X0[k, PAD + 8 * g:PAD + 8 * g + 8, :])

    shares = [send(G.at[mc], G.at[mc], g_s.at[i - 1], g_r.at[i - 1], (lax.rem(mc + i, C), me)) for i in range(1, C)]
    norms, outs = [], []
    for i, j in enumerate(others(A, me), 1):
        norms.append(send(Q.at[me], Q.at[me], q_s.at[i - 1], q_r.at[i - 1], (mc, j)))
        for h in range(m):
            n = (i - 1) * m + h
            outs.append(send(Y.at[j * m + h], out_ref.at[me, :, block_lanes[h]], o_s.at[n], o_r.at[n], (mc, j)))

    def gradient(h):
        flow = G[0, h * degree:(h + 1) * degree, :]
        for i in range(1, C):
            flow = flow + G[i, h * degree:(h + 1) * degree, :]
        return flow - cap_ref[:, block_lanes[h]]

    def sweep(t):
        read = lax.rem(t, 2)
        for g in range(groups):
            base = PAD + 8 * g - REACH

            def relax(best, other, start, index, weight, second, p):
                idx = index[g, p]
                w = weight[g, p]
                for k in range(rows):
                    got = jnp.take_along_axis(X[read, k, pl.ds(start, 8), :], idx, axis=1,
                                              mode="promise_in_bounds")
                    best[k] = jnp.minimum(best[k], got + w)
                    if second is not None:
                        other[k] = jnp.minimum(other[k], got + second[g, p])

            best = [X[read, k, PAD + 8 * g:PAD + 8 * g + 8, :] for k in range(rows)]
            other = [jnp.full((8, LANES), jnp.inf, jnp.float32)] * rows
            for o in range(OFFS):
                for i in range(FIXED):
                    relax(best, other, o + base, PI, PW, PV, o * FIXED + i)
            if extra <= CHUNK:
                for p in range(extra):
                    relax(best, other, OFF[g, p] + base, EI, EW, None, p)
            else:
                def more(c, best):
                    best = list(best)
                    for n in range(CHUNK):
                        relax(best, None, OFF[g, c * CHUNK + n] + base, EI, EW, None, c * CHUNK + n)
                    return tuple(best)
                best = lax.fori_loop(0, extra // CHUNK, more, tuple(best))
            for k in range(rows):
                put(X.at[1 - read, k], g, groups, jnp.minimum(best[k], pltpu.roll(other[k], HALF, 1)))

    def one(t, _):
        @pl.when(t == MEET)
        def _():
            wait_peers()
            for c in shares:
                c.start()

        @pl.when(t == SWEEPS - 1)
        def _():
            for c in shares:
                c.wait()
            Q[me] = sum(g * g for g in [gradient(h) for h in range(m)])
            for c in norms:
                c.start()

        sweep(t)
        return 0

    lax.fori_loop(0, SWEEPS, one, 0)

    for g in range(groups):
        for k in range(rows):
            Y[8 * g:8 * g + 8, k, :] = X[SWEEPS % 2, k, PAD + 8 * g:PAD + 8 * g + 8, :]
    for c in outs:
        c.start()
    for h in range(m):
        out_ref[me, :, block_lanes[h]] = Y[me * m + h]
    for c in norms:
        c.wait()
    square = Q[0]
    for i in range(1, A):
        square = square + Q[i]
    scale_root = jnp.sqrt(jnp.sum(square) / (degree * node_count) + eps_value)
    for h in range(m):
        newp_ref[:, block_lanes[h]] = jnp.maximum(
            price_ref[:, block_lanes[h]] + step_size * gradient(h) / scale_root, 0.0)
    for c in outs:
        c.wait()


def store_kernel(out_ref, newp_ref, out_hbm, newp_hbm, sem):
    copies = [pltpu.make_async_copy(out_ref, out_hbm, sem.at[0]), pltpu.make_async_copy(newp_ref, newp_hbm, sem.at[1])]
    for c in copies:
        c.start()
    for c in copies:
        c.wait()


def extras_of(degree):
    return OFFS * (degree - FIXED)


def shards(A, C, prev_dist, source_node, arc_tail, base_cost, arc_price, capacity, path_arcs, demand):
    commodities, span = prev_dist.shape
    degree = arc_tail.shape[0]
    rows = commodities // A
    m = span // LANES
    NB = A * m
    assert NB % 8 == 0 and degree >= 2 * FIXED and extras_of(degree) % CHUNK == 0
    f32, i32 = jnp.float32, jnp.int32
    groups = NB // 8
    extras = extras_of(degree)
    pitch = NB + 2 * PAD + (8 if (NB // 8) % 2 == 0 else 0)
    vmem = pl.BlockSpec(memory_space=pltpu.VMEM)
    smem = pl.BlockSpec(memory_space=pltpu.SMEM)
    hbm = pl.BlockSpec(memory_space=pltpu.HBM)
    sems = pltpu.SemaphoreType.DMA
    kept_words = (rows * (NB + 2 * PAD) + 16 * groups * degree + 8 * groups * OFFS * (2 + 3 * FIXED)) * LANES
    limit = 64_600_000 - 4 * kept_words
    X0, KT, WW, COUNT, CAP, PI, PW, PV, flow, price, cap = pl.pallas_call(
        functools.partial(gather_kernel, A, C, m),
        out_shape=(pltpu.VMEM((rows, NB + 2 * PAD, LANES), f32), pltpu.VMEM((groups, degree, 8, LANES), i32),
                   pltpu.VMEM((groups, degree, 8, LANES), f32), pltpu.VMEM((groups, OFFS, 8, LANES), i32),
                   pltpu.VMEM((groups, OFFS, 8, LANES), i32),
                   pltpu.VMEM((groups, OFFS * FIXED, 8, LANES), i32),
                   pltpu.VMEM((groups, OFFS * FIXED, 8, LANES), f32),
                   pltpu.VMEM((groups, OFFS * FIXED, 8, LANES), f32), pltpu.VMEM((m * degree, LANES), f32),
                   pltpu.VMEM((degree, span), f32), pltpu.VMEM((degree, span), f32)),
        in_specs=[smem] * 2 + [hbm] * 6,
        out_specs=(vmem,) * 11,
        scratch_shapes=[
            pltpu.VMEM((NB, rows, LANES), f32),
            pltpu.VMEM((A, rows, span), f32),
            pltpu.VMEM((degree, span), i32),
            pltpu.VMEM((degree, span), f32),
            pltpu.VMEM(path_arcs.shape, i32),
            pltpu.VMEM((NB, degree, LANES), i32),
            pltpu.VMEM((NB, degree, LANES), f32),
            pltpu.VMEM((A, m * degree, LANES), f32),
            pltpu.VMEM((A, m * degree, LANES), f32),
        ] + [sems((6,))] + [sems(((A - 1) * m,))] * 2 + [sems((A - 1,))] * 6,
        compiler_params=pltpu.CompilerParams(collective_id=0, has_side_effects=True, vmem_limit_bytes=limit),
    )(source_node, demand, prev_dist.reshape(A, rows, span), arc_tail, base_cost, arc_price, capacity, path_arcs)
    local = pltpu.CompilerParams(vmem_limit_bytes=24 * 2**20)
    EI, EW, OFF, choice = pl.pallas_call(
        list_kernel,
        out_shape=(pltpu.VMEM((groups, extras, 8, LANES), i32), pltpu.VMEM((groups, extras, 8, LANES), f32),
                   jax.ShapeDtypeStruct((groups, extras), i32), jax.ShapeDtypeStruct((1,), i32)),
        in_specs=[vmem] * 4,
        out_specs=(vmem, vmem, smem, smem),
        compiler_params=local,
    )(KT, WW, COUNT, CAP)

    def branch(n, extra):
        return lambda *operands: pl.pallas_call(
            functools.partial(sweep_kernel, A, C, m, extra),
            out_shape=(pltpu.VMEM((A, rows, span), f32), pltpu.VMEM((degree, span), f32)),
            in_specs=[smem] + [vmem] * 9,
            out_specs=(vmem, vmem),
            scratch_shapes=[
                pltpu.VMEM((2, rows, pitch, LANES), f32),
                pltpu.VMEM((NB, rows, LANES), f32),
                pltpu.VMEM((C, m * degree, LANES), f32),
                pltpu.VMEM((A, degree, LANES), f32),
            ] + [sems((C - 1,))] * 2 + [sems((A - 1,))] * 2 + [sems(((A - 1) * m,))] * 2,
            compiler_params=pltpu.CompilerParams(collective_id=1 + n, has_side_effects=True,
                                                 vmem_limit_bytes=24 * 2**20),
        )(*operands)

    out, new_price = lax.switch(choice[0], [branch(n, extra) for n, extra in enumerate(BUCKETS + (extras,))],
                                OFF, X0, PI, PW, PV, EI, EW, flow, price, cap)
    out, new_price = pl.pallas_call(
        store_kernel,
        out_shape=(jax.ShapeDtypeStruct(out.shape, f32), jax.ShapeDtypeStruct(new_price.shape, f32)),
        in_specs=[vmem] * 2,
        out_specs=(hbm, hbm),
        scratch_shapes=[sems((2,))],
        compiler_params=pltpu.CompilerParams(vmem_limit_bytes=24 * 2**20),
    )(out, new_price)
    return (out.reshape(commodities, span), new_price)


def solution(mesh):
    in_specs = (
        P("comm", "arc"),
        P("comm"),
        P(None, "arc"),
        P(None, "arc"),
        P(None, "arc"),
        P(None, "arc"),
        P(("comm", "arc"), None),
        P(("comm", "arc")),
    )
    out_specs = (P("comm", "arc"), P(None, "arc"))
    body = functools.partial(shards, mesh.shape["arc"], mesh.shape["comm"])
    return jax.shard_map(body, mesh=mesh, in_specs=in_specs, out_specs=out_specs, check_vma=False)
```

```python
import functools

import jax
import jax.numpy as jnp
from jax import lax
from jax.experimental import pallas as pl
from jax.experimental.pallas import tpu as pltpu
from jax.sharding import PartitionSpec as P

SWEEPS = 8
LANES = 128
REACH = 2
OFFS = 2 * REACH + 1
PAD = 8
FIXED = 7
BUCKETS = (2, 5)
CHUNK = 5
MEET = 2
HALF = LANES // 2

step_size = 0.25
eps_value = 1e-06
MESH_ID = pl.DeviceIdType.MESH


def send(src, dst, ss, rs, dev):
    return pltpu.make_async_remote_copy(src_ref=src, dst_ref=dst, send_sem=ss, recv_sem=rs,
                                        device_id=dev, device_id_type=MESH_ID)


def flip(index, bits, size):
    return sum(lax.rem(index // b + (bits // b) % 2, 2) * b for b in (1 << n for n in range((size - 1).bit_length())))


def others(A, me):
    chips = A // 2
    assert chips & (chips - 1) == 0
    far = sorted(range(1, chips), key=lambda bits: -bits.bit_count())
    core = lax.rem(me, 2)
    out = [2 * flip(me // 2, bits, chips) + lax.rem(core + c, 2) for bits in far for c in (0, 1)]
    return out + [2 * (me // 2) + 1 - core]


def greet(A, C, me, mc, along_comm):
    barrier = pltpu.get_barrier_semaphore()
    for i in range(1, A):
        pl.semaphore_signal(barrier, inc=1, device_id=(mc, lax.rem(me + i, A)), device_id_type=MESH_ID)
    for i in range(1, C if along_comm else 1):
        pl.semaphore_signal(barrier, inc=1, device_id=(lax.rem(mc + i, C), me), device_id_type=MESH_ID)
    return lambda: pl.semaphore_wait(barrier, A - 1 + (C - 1 if along_comm else 0))


def gather_kernel(A, C, m,
                  source_ref, demand_ref, dist_hbm, tail_hbm, cost_hbm, price_hbm, cap_hbm, path_hbm,
                  X0, KT, WW, COUNT, CAP, PI, PW, PV, EI, EW, flow_ref, price_ref, cap_ref, OFF, choice,
                  D, dist_ref, tail_ref, cost_ref, path_ref,
                  T, W, F, RF,
                  in_s, d_s, d_r, t_s, t_r, w_s, w_r, f_s, f_r):
    degree, span = tail_ref.shape
    NB = A * m
    chips = A // 2
    node_count = NB * LANES
    groups = NB // 8
    me = lax.axis_index("arc")
    mc = lax.axis_index("comm")
    chip, core = me // 2, lax.rem(me, 2)
    twin = 2 * chip + 1 - core
    block_lanes = [slice(h * LANES, (h + 1) * LANES) for h in range(m)]

    pairs = ((tail_hbm, tail_ref), (cost_hbm, cost_ref), (price_hbm, price_ref), (dist_hbm, dist_ref),
             (path_hbm, path_ref), (cap_hbm, cap_ref))
    loads = [pltpu.make_async_copy(src, dst, in_s.at[i]) for i, (src, dst) in enumerate(pairs)]
    for c in loads:
        c.start()
    wait_peers = greet(A, C, me, mc, False)
    for c in loads[:3]:
        c.wait()
    for h in range(m):
        W[me * m + h] = cost_ref[:, block_lanes[h]] + price_ref[:, block_lanes[h]]
        T[me * m + h] = tail_ref[:, block_lanes[h]]
    wait_peers()

    def share(owner, n, dev):
        at = pl.ds(owner * m, m)
        return [send(T.at[at], T.at[at], t_s.at[n], t_r.at[n], dev),
                send(W.at[at], W.at[at], w_s.at[n], w_r.at[n], dev)]

    far = []
    for i in range(1, chips):
        far += share(me, i - 1, (mc, 2 * flip(chip, i, chips) + core))
    near = share(me, chips - 1, (mc, twin))
    for c in far + near:
        c.start()
    loads[3].wait()
    dists = []
    for i, j in enumerate(others(A, me), 1):
        for h in range(m):
            n = (i - 1) * m + h
            dists.append(send(dist_ref.at[j, :, block_lanes[h]], D.at[me * m + h], d_s.at[n], d_r.at[n], (mc, j)))
    for c in dists:
        c.start()
    for h in range(m):
        D[me * m + h] = dist_ref[me, :, block_lanes[h]]
    for c in loads[4:]:
        c.wait()

    total_rows = NB * degree
    shift_nodes = (node_count - 1).bit_length()
    assert 1 << shift_nodes == node_count
    path = path_ref[...]
    slot_of = path >> shift_nodes
    node_of = path & (node_count - 1)
    row_of = (node_of >> 7) * degree + slot_of
    lane_of = node_of & (LANES - 1)
    row_iota = lax.broadcasted_iota(jnp.int32, (total_rows, LANES), 0)
    lane_iota = lax.broadcasted_iota(jnp.int32, (LANES, LANES), 0)
    acc = jnp.zeros((total_rows, LANES), jnp.float32)
    for k in range(path.shape[0]):
        hi = jnp.where(row_iota == row_of[k:k + 1, :], 1.0, 0.0).astype(jnp.bfloat16)
        lo = jnp.where(lane_iota == lane_of[k:k + 1, :], 1.0, 0.0).astype(jnp.bfloat16)
        count = lax.dot_general(hi, lo, (((1,), (1,)), ((), ())), preferred_element_type=jnp.float32)
        acc = acc + count * demand_ref[k]
    F[...] = acc.reshape(F.shape)

    flows = []
    for i, j in enumerate(others(A, me), 1):
        flows.append(send(F.at[j], RF.at[me], f_s.at[i - 1], f_r.at[i - 1], (mc, j)))
    for c in flows:
        c.start()
    passed = []
    for i in range(1, chips):
        for c in far[2 * (i - 1):2 * i]:
            c.wait()
        owner = 2 * flip(chip, i, chips) + core
        onward = share(owner, chips - 1 + i, (mc, twin))
        for c in onward:
            c.start()
        passed += onward

    for c in near + passed:
        c.wait()

    sub = lax.broadcasted_iota(jnp.int32, (8, LANES), 0)
    for g in range(groups):
        count = [jnp.zeros((8, LANES), jnp.int32)] * OFFS
        for s in range(degree):
            tail = T[8 * g:8 * g + 8, s, :]
            rel = (tail >> 7) - (8 * g + sub) + REACH
            rel = jnp.where(rel < 0, rel + NB, rel)
            rel = jnp.where(rel >= NB, rel - NB, rel)
            rank = count[0]
            for o in range(1, OFFS):
                rank = jnp.where(rel == o, count[o], rank)
            count = [c + jnp.where(rel == o, 1, 0) for o, c in enumerate(count)]
            KT[g, s] = ((rel * degree + rank) << 7) + (tail & (LANES - 1))
            WW[g, s] = W[8 * g:8 * g + 8, s, :]
        for o in range(OFFS):
            free = FIXED - jnp.minimum(pltpu.roll(count[o], HALF, 1), FIXED)
            CAP[g, o] = FIXED + free
            COUNT[g, o] = jnp.maximum(count[o] - FIXED - free, 0)

    def build(o, _):
        for g in range(groups):
            kts = [KT[g, s] for s in range(degree)]
            ranks = [(kt >> 7) - o * degree for kt in kts]
            weights = [WW[g, s] for s in range(degree)]

            def find(rank):
                kept = jnp.zeros((8, LANES), jnp.int32)
                weight = jnp.full((8, LANES), jnp.inf, jnp.float32)
                for s in range(rank, degree):
                    hit = ranks[s] == rank
                    kept = jnp.where(hit, kts[s], kept)
                    weight = jnp.where(hit, weights[s], weight)
                return kept, weight

            for i in range(FIXED):
                own_kept, own_weight = find(i)
                far_kept, far_weight = [pltpu.roll(x, HALF, 1) for x in find(2 * FIXED - 1 - i)]
                mine = own_weight < jnp.inf
                p = o * FIXED + i
                PI[g, p] = jnp.where(mine, own_kept, far_kept) & (LANES - 1)
                PW[g, p] = own_weight
                PV[g, p] = jnp.where(mine, jnp.inf, far_weight)
        return 0

    lax.fori_loop(0, OFFS, build, 0)

    ends = [ends_of(COUNT, g) for g in range(groups)]
    for g in range(groups):
        for p in range(BUCKETS[-1]):
            EI[g, p], EW[g, p], OFF[g, p] = leftover(KT, WW, CAP, ends[g], g, p, degree)
    most = functools.reduce(jnp.maximum, [end[-1] for end in ends])
    choice[0] = sum(jnp.where(most > size, 1, 0) for size in BUCKETS)

    for c in dists:
        c.wait()
    lane = lax.broadcasted_iota(jnp.int32, (8, LANES), 1)
    for g in range(groups):
        node = (8 * g + sub) * LANES + lane
        for k in range(D.shape[1]):
            old = D[8 * g:8 * g + 8, k, :]
            put(X0.at[k], g, groups, jnp.where(node == source_ref[me * D.shape[1] + k], 0.0, old))
    for c in flows:
        c.wait()
    total = F[me]
    for i in range(1, A):
        total = total + RF[lax.rem(me + i, A)]
    flow_ref[...] = total


def arc_of(KT, WW, g, key, degree):
    kept = jnp.zeros((8, LANES), jnp.int32)
    weight = jnp.full((8, LANES), jnp.inf, jnp.float32)
    for s in range(degree):
        kt = KT[g, s]
        hit = (kt >> 7) == key
        kept = jnp.where(hit, kt, kept)
        weight = jnp.where(hit, WW[g, s], weight)
    return kept & (LANES - 1), weight


def ends_of(COUNT, g):
    ends = [jnp.max(COUNT[g, 0])]
    for o in range(1, OFFS):
        ends.append(ends[-1] + jnp.max(COUNT[g, o]))
    return ends


def leftover(KT, WW, CAP, ends, g, p, degree):
    offset, start = 0, 0
    rank = CAP[g, 0]
    for o in range(1, OFFS):
        later = p >= ends[o - 1]
        offset = jnp.where(later, o, offset)
        start = jnp.where(later, ends[o - 1], start)
        rank = jnp.where(later, CAP[g, o], rank)
    rank = rank + (p - start)
    key = jnp.where((rank < degree) & (p < ends[-1]), offset * degree + rank, -1)
    return *arc_of(KT, WW, g, key, degree), offset


def put(row, g, groups, value):
    row[PAD + 8 * g:PAD + 8 * g + 8, :] = value
    if g == 0:
        row[PAD + 8 * groups:PAD + 8 * groups + REACH, :] = value[:REACH]
    if g == groups - 1:
        row[PAD - REACH:PAD, :] = value[8 - REACH:]


def sweep_kernel(A, C, m, extra,
                 OFF, X0, KT, WW, COUNT, CAP, PI, PW, PV, EI, EW, flow_ref, price_ref, cap_ref,
                 out_ref, newp_ref,
                 X, Y, G, Q,
                 g_s, g_r, q_s, q_r, o_s, o_r, *lists):
    rows = X0.shape[0]
    groups = PI.shape[0]
    degree, span = price_ref.shape
    node_count = A * m * LANES
    me = lax.axis_index("arc")
    mc = lax.axis_index("comm")
    block_lanes = [slice(h * LANES, (h + 1) * LANES) for h in range(m)]

    wait_peers = greet(A, C, me, mc, True)
    G[mc] = flow_ref[...]
    for g in range(groups):
        for k in range(rows):
            put(X.at[0, k], g, groups, X0[k, PAD + 8 * g:PAD + 8 * g + 8, :])

    if lists:
        EI, EW, OFF = lists
        for g in range(groups):
            ends = ends_of(COUNT, g)

            def fill(p, _, g=g, ends=ends):
                EI[g, p], EW[g, p], OFF[g, p] = leftover(KT, WW, CAP, ends, g, p, degree)
                return 0
            lax.fori_loop(0, extra, fill, 0)

    shares = [send(G.at[mc], G.at[mc], g_s.at[i - 1], g_r.at[i - 1], (lax.rem(mc + i, C), me)) for i in range(1, C)]
    norms = [send(Q.at[me], Q.at[me], q_s.at[i - 1], q_r.at[i - 1], (mc, j)) for i, j in enumerate(others(A, me), 1)]

    def gradient(h):
        flow = G[0, h * degree:(h + 1) * degree, :]
        for i in range(1, C):
            flow = flow + G[i, h * degree:(h + 1) * degree, :]
        return flow - cap_ref[:, block_lanes[h]]

    def relaxed(read, g):
        base = 8 * g + (PAD - REACH)

        def relax(best, other, start, index, weight, second, p):
            idx = index[g, p]
            w = weight[g, p]
            for k in range(rows):
                got = jnp.take_along_axis(X[read, k, pl.ds(start, 8), :], idx, axis=1,
                                          mode="promise_in_bounds")
                best[k] = jnp.minimum(best[k], got + w)
                if second is not None:
                    other[k] = jnp.minimum(other[k], got + second[g, p])

        best = [X[read, k, pl.ds(base + REACH, 8), :] for k in range(rows)]
        other = [jnp.full((8, LANES), jnp.inf, jnp.float32)] * rows
        for o in range(OFFS):
            for i in range(FIXED):
                relax(best, other, base + o, PI, PW, PV, o * FIXED + i)
        if not lists:
            for p in range(extra):
                relax(best, other, OFF[g, p] + base, EI, EW, None, p)
        else:
            def more(c, best):
                best = list(best)
                for n in range(CHUNK):
                    relax(best, None, OFF[g, c * CHUNK + n] + base, EI, EW, None, c * CHUNK + n)
                return tuple(best)
            best = lax.fori_loop(0, extra // CHUNK, more, tuple(best))
        return [jnp.minimum(best[k], pltpu.roll(other[k], HALF, 1)) for k in range(rows)]

    def one(t, _):
        @pl.when(t == MEET)
        def _():
            wait_peers()
            for c in shares:
                c.start()

        read = lax.rem(t, 2)
        for g in range(groups):
            for k, value in enumerate(relaxed(read, g)):
                put(X.at[1 - read, k], g, groups, value)
        return 0

    lax.fori_loop(0, SWEEPS - 1, one, 0)

    for c in shares:
        c.wait()
    Q[me] = sum(g * g for g in [gradient(h) for h in range(m)])
    for c in norms:
        c.start()

    per = 8 // m
    seat = lax.rem(me, per)
    outs = []
    for n in range(groups):
        g = lax.rem(me // per + 1 + n, groups)
        for k, value in enumerate(relaxed((SWEEPS - 1) % 2, g)):
            Y[pl.ds(8 * g, 8), k, :] = value
        turns = [(per // 2 + q) % per for q in range(per)]
        ready = []
        for q in turns:
            if n == groups - 1 and q == 0:
                continue
            j = g * per + lax.rem(seat + q, per)
            for h in range(m):
                at = len(outs) + len(ready)
                ready.append(send(Y.at[j * m + h], out_ref.at[me, :, block_lanes[h]], o_s.at[at], o_r.at[at], (mc, j)))
        for c in ready:
            c.start()
        outs += ready
    for h in range(m):
        out_ref[me, :, block_lanes[h]] = Y[me * m + h]
    for c in norms:
        c.wait()
    square = Q[0]
    for i in range(1, A):
        square = square + Q[i]
    scale_root = jnp.sqrt(jnp.sum(square) / (degree * node_count) + eps_value)
    for h in range(m):
        newp_ref[:, block_lanes[h]] = jnp.maximum(
            price_ref[:, block_lanes[h]] + step_size * gradient(h) / scale_root, 0.0)
    for c in outs:
        c.wait()


def store_kernel(out_ref, newp_ref, out_hbm, newp_hbm, sem):
    copies = [pltpu.make_async_copy(out_ref, out_hbm, sem.at[0]), pltpu.make_async_copy(newp_ref, newp_hbm, sem.at[1])]
    for c in copies:
        c.start()
    for c in copies:
        c.wait()


def extras_of(degree):
    return OFFS * (degree - FIXED)


def shards(A, C, prev_dist, source_node, arc_tail, base_cost, arc_price, capacity, path_arcs, demand):
    commodities, span = prev_dist.shape
    degree = arc_tail.shape[0]
    rows = commodities // A
    m = span // LANES
    NB = A * m
    assert NB % 8 == 0 and 8 % m == 0 and A % (8 // m) == 0 and degree >= 2 * FIXED and extras_of(degree) % CHUNK == 0
    f32, i32 = jnp.float32, jnp.int32
    groups = NB // 8
    extras = extras_of(degree)
    pitch = NB + 2 * PAD + (8 if (NB // 8) % 2 == 0 else 0)
    vmem = pl.BlockSpec(memory_space=pltpu.VMEM)
    smem = pl.BlockSpec(memory_space=pltpu.SMEM)
    hbm = pl.BlockSpec(memory_space=pltpu.HBM)
    sems = pltpu.SemaphoreType.DMA
    kept_words = (rows * (NB + 2 * PAD) + 16 * groups * degree + 8 * groups * (OFFS * (2 + 3 * FIXED) + 2 * BUCKETS[-1])) * LANES
    limit = 64_600_000 - 4 * kept_words
    X0, KT, WW, COUNT, CAP, PI, PW, PV, EI, EW, flow, price, cap, OFF, choice = pl.pallas_call(
        functools.partial(gather_kernel, A, C, m),
        out_shape=(pltpu.VMEM((rows, NB + 2 * PAD, LANES), f32), pltpu.VMEM((groups, degree, 8, LANES), i32),
                   pltpu.VMEM((groups, degree, 8, LANES), f32), pltpu.VMEM((groups, OFFS, 8, LANES), i32),
                   pltpu.VMEM((groups, OFFS, 8, LANES), i32),
                   pltpu.VMEM((groups, OFFS * FIXED, 8, LANES), i32),
                   pltpu.VMEM((groups, OFFS * FIXED, 8, LANES), f32),
                   pltpu.VMEM((groups, OFFS * FIXED, 8, LANES), f32),
                   pltpu.VMEM((groups, BUCKETS[-1], 8, LANES), i32), pltpu.VMEM((groups, BUCKETS[-1], 8, LANES), f32),
                   pltpu.VMEM((m * degree, LANES), f32),
                   pltpu.VMEM((degree, span), f32), pltpu.VMEM((degree, span), f32),
                   jax.ShapeDtypeStruct((groups, BUCKETS[-1]), i32), jax.ShapeDtypeStruct((1,), i32)),
        in_specs=[smem] * 2 + [hbm] * 6,
        out_specs=(vmem,) * 13 + (smem,) * 2,
        scratch_shapes=[
            pltpu.VMEM((NB, rows, LANES), f32),
            pltpu.VMEM((A, rows, span), f32),
            pltpu.VMEM((degree, span), i32),
            pltpu.VMEM((degree, span), f32),
            pltpu.VMEM(path_arcs.shape, i32),
            pltpu.VMEM((NB, degree, LANES), i32),
            pltpu.VMEM((NB, degree, LANES), f32),
            pltpu.VMEM((A, m * degree, LANES), f32),
            pltpu.VMEM((A, m * degree, LANES), f32),
        ] + [sems((6,))] + [sems(((A - 1) * m,))] * 2 + [sems((A - 1,))] * 6,
        compiler_params=pltpu.CompilerParams(collective_id=0, has_side_effects=True, vmem_limit_bytes=limit),
    )(source_node, demand, prev_dist.reshape(A, rows, span), arc_tail, base_cost, arc_price, capacity, path_arcs)
    def branch(n, extra):
        return lambda *operands: pl.pallas_call(
            functools.partial(sweep_kernel, A, C, m, extra),
            out_shape=(pltpu.VMEM((A, rows, span), f32), pltpu.VMEM((degree, span), f32)),
            in_specs=[smem] + [vmem] * 13,
            out_specs=(vmem, vmem),
            scratch_shapes=[
                pltpu.VMEM((2, rows, pitch, LANES), f32),
                pltpu.VMEM((NB, rows, LANES), f32),
                pltpu.VMEM((C, m * degree, LANES), f32),
                pltpu.VMEM((A, degree, LANES), f32),
            ] + [sems((C - 1,))] * 2 + [sems((A - 1,))] * 2 + [sems(((A - 1) * m,))] * 2 + ([] if extra in BUCKETS else [
                pltpu.VMEM((groups, extra, 8, LANES), i32),
                pltpu.VMEM((groups, extra, 8, LANES), f32),
                pltpu.SMEM((groups, extra), i32),
            ]),
            compiler_params=pltpu.CompilerParams(collective_id=1 + n, has_side_effects=True, vmem_limit_bytes=24 * 2**20),
        )(*operands)

    out, new_price = lax.switch(choice[0], [branch(n, extra) for n, extra in enumerate(BUCKETS + (extras,))],
                                OFF, X0, KT, WW, COUNT, CAP, PI, PW, PV, EI, EW, flow, price, cap)
    out, new_price = pl.pallas_call(
        store_kernel,
        out_shape=(jax.ShapeDtypeStruct(out.shape, f32), jax.ShapeDtypeStruct(new_price.shape, f32)),
        in_specs=[vmem] * 2,
        out_specs=(hbm, hbm),
        scratch_shapes=[sems((2,))],
        compiler_params=pltpu.CompilerParams(vmem_limit_bytes=24 * 2**20),
    )(out, new_price)
    return (out.reshape(commodities, span), new_price)


def solution(mesh):
    in_specs = (
        P("comm", "arc"),
        P("comm"),
        P(None, "arc"),
        P(None, "arc"),
        P(None, "arc"),
        P(None, "arc"),
        P(("comm", "arc"), None),
        P(("comm", "arc")),
    )
    out_specs = (P("comm", "arc"), P(None, "arc"))
    body = functools.partial(shards, mesh.shape["arc"], mesh.shape["comm"])
    return jax.shard_map(body, mesh=mesh, in_specs=in_specs, out_specs=out_specs, check_vma=False)
```

```python
import functools

import jax
import jax.numpy as jnp
from jax import lax
from jax.experimental import pallas as pl
from jax.experimental.pallas import tpu as pltpu
from jax.sharding import PartitionSpec as P

SWEEPS = 8
LANES = 128
REACH = 2
OFFS = 2 * REACH + 1
PAD = 8
FIXED = 7
BUCKETS = (2, 5)
CHUNK = 5
MEET = 2
HALF = LANES // 2

step_size = 0.25
eps_value = 1e-06
MESH_ID = pl.DeviceIdType.MESH


def send(src, dst, ss, rs, dev):
    return pltpu.make_async_remote_copy(src_ref=src, dst_ref=dst, send_sem=ss, recv_sem=rs,
                                        device_id=dev, device_id_type=MESH_ID)


def flip(index, bits, size):
    return sum(lax.rem(index // b + (bits // b) % 2, 2) * b for b in (1 << n for n in range((size - 1).bit_length())))


def others(A, me):
    chips = A // 2
    assert chips & (chips - 1) == 0
    far = sorted(range(1, chips), key=lambda bits: -bits.bit_count())
    core = lax.rem(me, 2)
    out = [2 * flip(me // 2, bits, chips) + lax.rem(core + c, 2) for bits in far for c in (0, 1)]
    return out + [2 * (me // 2) + 1 - core]


def greet(A, C, me, mc, along_comm):
    barrier = pltpu.get_barrier_semaphore()
    for i in range(1, A):
        pl.semaphore_signal(barrier, inc=1, device_id=(mc, lax.rem(me + i, A)), device_id_type=MESH_ID)
    for i in range(1, C if along_comm else 1):
        pl.semaphore_signal(barrier, inc=1, device_id=(lax.rem(mc + i, C), me), device_id_type=MESH_ID)
    return lambda: pl.semaphore_wait(barrier, A - 1 + (C - 1 if along_comm else 0))


def gather_kernel(A, C, m,
                  source_ref, demand_ref, dist_hbm, tail_hbm, cost_hbm, price_hbm, cap_hbm, path_hbm,
                  X0, KT, WW, COUNT, CAP, PI, PW, PV, EI, EW, flow_ref, price_ref, cap_ref, OFF, choice,
                  D, dist_ref, tail_ref, cost_ref, path_ref,
                  T, W, F, RF,
                  in_s, d_s, d_r, t_s, t_r, w_s, w_r, f_s, f_r):
    degree, span = tail_ref.shape
    NB = A * m
    chips = A // 2
    node_count = NB * LANES
    groups = NB // 8
    me = lax.axis_index("arc")
    mc = lax.axis_index("comm")
    chip, core = me // 2, lax.rem(me, 2)
    twin = 2 * chip + 1 - core
    block_lanes = [slice(h * LANES, (h + 1) * LANES) for h in range(m)]

    pairs = ((tail_hbm, tail_ref), (cost_hbm, cost_ref), (price_hbm, price_ref), (dist_hbm, dist_ref),
             (path_hbm, path_ref), (cap_hbm, cap_ref))
    loads = [pltpu.make_async_copy(src, dst, in_s.at[i]) for i, (src, dst) in enumerate(pairs)]
    for c in loads:
        c.start()
    wait_peers = greet(A, C, me, mc, False)
    for c in loads[:3]:
        c.wait()
    for h in range(m):
        at = pl.ds(pl.multiple_of((me * m + h) * degree, degree), degree)
        W[at, :] = cost_ref[:, block_lanes[h]] + price_ref[:, block_lanes[h]]
        T[at, :] = tail_ref[:, block_lanes[h]]
    wait_peers()

    def share(owner, n, dev):
        at = pl.ds(pl.multiple_of(owner * (m * degree), m * degree), m * degree)
        return [send(T.at[at], T.at[at], t_s.at[n], t_r.at[n], dev),
                send(W.at[at], W.at[at], w_s.at[n], w_r.at[n], dev)]

    far = []
    for i in range(1, chips):
        far += share(me, i - 1, (mc, 2 * flip(chip, i, chips) + core))
    near = share(me, chips - 1, (mc, twin))
    for c in far + near:
        c.start()
    loads[3].wait()
    dists = []
    for i, j in enumerate(others(A, me), 1):
        for h in range(m):
            n = (i - 1) * m + h
            dists.append(send(dist_ref.at[j, :, block_lanes[h]], D.at[me * m + h], d_s.at[n], d_r.at[n], (mc, j)))
    for c in dists:
        c.start()
    for h in range(m):
        D[me * m + h] = dist_ref[me, :, block_lanes[h]]
    for c in loads[4:]:
        c.wait()

    total_rows = NB * degree
    shift_nodes = (node_count - 1).bit_length()
    assert 1 << shift_nodes == node_count
    path = path_ref[...]
    slot_of = path >> shift_nodes
    node_of = path & (node_count - 1)
    row_of = (node_of >> 7) * degree + slot_of
    lane_of = node_of & (LANES - 1)
    row_iota = lax.broadcasted_iota(jnp.int32, (total_rows, LANES), 0)
    lane_iota = lax.broadcasted_iota(jnp.int32, (LANES, LANES), 0)
    acc = jnp.zeros((total_rows, LANES), jnp.float32)
    for k in range(path.shape[0]):
        hi = jnp.where(row_iota == row_of[k:k + 1, :], 1.0, 0.0).astype(jnp.bfloat16)
        lo = jnp.where(lane_iota == lane_of[k:k + 1, :], 1.0, 0.0).astype(jnp.bfloat16)
        count = lax.dot_general(hi, lo, (((1,), (1,)), ((), ())), preferred_element_type=jnp.float32)
        acc = acc + count * demand_ref[k]
    F[...] = acc.reshape(F.shape)

    flows = []
    for i, j in enumerate(others(A, me), 1):
        flows.append(send(F.at[j], RF.at[me], f_s.at[i - 1], f_r.at[i - 1], (mc, j)))
    for c in flows:
        c.start()
    passed = []
    for i in range(1, chips):
        for c in far[2 * (i - 1):2 * i]:
            c.wait()
        owner = 2 * flip(chip, i, chips) + core
        onward = share(owner, chips - 1 + i, (mc, twin))
        for c in onward:
            c.start()
        passed += onward

    for c in near + passed:
        c.wait()

    sub = lax.broadcasted_iota(jnp.int32, (8, LANES), 0)
    for g in range(groups):
        count = [jnp.zeros((8, LANES), jnp.int32)] * OFFS
        for s in range(degree):
            tail = T[pl.ds(8 * g * degree + s, 8, stride=degree), :]
            rel = (tail >> 7) - (8 * g + sub) + REACH
            rel = jnp.where(rel < 0, rel + NB, rel)
            rel = jnp.where(rel >= NB, rel - NB, rel)
            rank = count[0]
            for o in range(1, OFFS):
                rank = jnp.where(rel == o, count[o], rank)
            count = [c + jnp.where(rel == o, 1, 0) for o, c in enumerate(count)]
            KT[g, s] = ((rel * degree + rank) << 7) + (tail & (LANES - 1))
            WW[g, s] = W[pl.ds(8 * g * degree + s, 8, stride=degree), :]
        for o in range(OFFS):
            free = FIXED - jnp.minimum(pltpu.roll(count[o], HALF, 1), FIXED)
            CAP[g, o] = FIXED + free
            COUNT[g, o] = jnp.maximum(count[o] - FIXED - free, 0)

    def build(o, _):
        for g in range(groups):
            kts = [KT[g, s] for s in range(degree)]
            ranks = [(kt >> 7) - o * degree for kt in kts]
            weights = [WW[g, s] for s in range(degree)]

            def find(rank):
                kept = jnp.zeros((8, LANES), jnp.int32)
                weight = jnp.full((8, LANES), jnp.inf, jnp.float32)
                for s in range(rank, degree):
                    hit = ranks[s] == rank
                    kept = jnp.where(hit, kts[s], kept)
                    weight = jnp.where(hit, weights[s], weight)
                return kept, weight

            for i in range(FIXED):
                own_kept, own_weight = find(i)
                far_kept, far_weight = [pltpu.roll(x, HALF, 1) for x in find(2 * FIXED - 1 - i)]
                mine = own_weight < jnp.inf
                p = o * FIXED + i
                PI[g, p] = jnp.where(mine, own_kept, far_kept) & (LANES - 1)
                PW[g, p] = own_weight
                PV[g, p] = jnp.where(mine, jnp.inf, far_weight)
        return 0

    lax.fori_loop(0, OFFS, build, 0)

    for c in dists:
        c.wait()
    ends = [ends_of(COUNT, g) for g in range(groups)]
    for g in range(groups):
        for p in range(BUCKETS[-1]):
            EI[g, p], EW[g, p], OFF[g, p] = leftover(KT, WW, CAP, ends[g], g, p, degree)
    most = functools.reduce(jnp.maximum, [end[-1] for end in ends])
    choice[0] = sum(jnp.where(most > size, 1, 0) for size in BUCKETS)

    lane = lax.broadcasted_iota(jnp.int32, (8, LANES), 1)
    for g in range(groups):
        node = (8 * g + sub) * LANES + lane
        for k in range(D.shape[1]):
            old = D[8 * g:8 * g + 8, k, :]
            put(X0.at[k], g, groups, jnp.where(node == source_ref[me * D.shape[1] + k], 0.0, old))
    for c in flows:
        c.wait()
    total = F[me]
    for i in range(1, A):
        total = total + RF[lax.rem(me + i, A)]
    flow_ref[...] = total


def arc_of(KT, WW, g, key, degree):
    kept = jnp.zeros((8, LANES), jnp.int32)
    weight = jnp.full((8, LANES), jnp.inf, jnp.float32)
    for s in range(degree):
        kt = KT[g, s]
        hit = (kt >> 7) == key
        kept = jnp.where(hit, kt, kept)
        weight = jnp.where(hit, WW[g, s], weight)
    return kept & (LANES - 1), weight


def ends_of(COUNT, g):
    ends = [jnp.max(COUNT[g, 0])]
    for o in range(1, OFFS):
        ends.append(ends[-1] + jnp.max(COUNT[g, o]))
    return ends


def leftover(KT, WW, CAP, ends, g, p, degree):
    offset, start = 0, 0
    rank = CAP[g, 0]
    for o in range(1, OFFS):
        later = p >= ends[o - 1]
        offset = jnp.where(later, o, offset)
        start = jnp.where(later, ends[o - 1], start)
        rank = jnp.where(later, CAP[g, o], rank)
    rank = rank + (p - start)
    key = jnp.where((rank < degree) & (p < ends[-1]), offset * degree + rank, -1)
    return *arc_of(KT, WW, g, key, degree), offset


def put(row, g, groups, value):
    row[PAD + 8 * g:PAD + 8 * g + 8, :] = value
    if g == 0:
        row[PAD + 8 * groups:PAD + 8 * groups + REACH, :] = value[:REACH]
    if g == groups - 1:
        row[PAD - REACH:PAD, :] = value[8 - REACH:]


def sweep_kernel(A, C, m, extra,
                 OFF, X0, KT, WW, COUNT, CAP, PI, PW, PV, EI, EW, flow_ref, price_ref, cap_ref,
                 out_ref, newp_ref,
                 X, Y, G, Q,
                 g_s, g_r, q_s, q_r, o_s, o_r, *lists):
    rows = X0.shape[0]
    groups = PI.shape[0]
    degree, span = price_ref.shape
    node_count = A * m * LANES
    me = lax.axis_index("arc")
    mc = lax.axis_index("comm")
    block_lanes = [slice(h * LANES, (h + 1) * LANES) for h in range(m)]

    wait_peers = greet(A, C, me, mc, True)
    G[mc] = flow_ref[...]
    for g in range(groups):
        for k in range(rows):
            put(X.at[0, k], g, groups, X0[k, PAD + 8 * g:PAD + 8 * g + 8, :])

    if lists:
        EI, EW, OFF = lists
        for g in range(groups):
            ends = ends_of(COUNT, g)

            def fill(p, _, g=g, ends=ends):
                EI[g, p], EW[g, p], OFF[g, p] = leftover(KT, WW, CAP, ends, g, p, degree)
                return 0
            lax.fori_loop(0, extra, fill, 0)

    shares = [send(G.at[mc], G.at[mc], g_s.at[i - 1], g_r.at[i - 1], (lax.rem(mc + i, C), me)) for i in range(1, C)]
    norms = [send(Q.at[me], Q.at[me], q_s.at[i - 1], q_r.at[i - 1], (mc, j)) for i, j in enumerate(others(A, me), 1)]

    def gradient(h):
        flow = G[0, h * degree:(h + 1) * degree, :]
        for i in range(1, C):
            flow = flow + G[i, h * degree:(h + 1) * degree, :]
        return flow - cap_ref[:, block_lanes[h]]

    def relaxed(read, g):
        base = 8 * g + (PAD - REACH)

        def relax(best, other, start, index, weight, second, p):
            idx = index[g, p]
            w = weight[g, p]
            for k in range(rows):
                got = jnp.take_along_axis(X[read, k, pl.ds(start, 8), :], idx, axis=1,
                                          mode="promise_in_bounds")
                best[k] = jnp.minimum(best[k], got + w)
                if second is not None:
                    other[k] = jnp.minimum(other[k], got + second[g, p])

        best = [X[read, k, pl.ds(base + REACH, 8), :] for k in range(rows)]
        other = [jnp.full((8, LANES), jnp.inf, jnp.float32)] * rows
        for o in range(OFFS):
            for i in range(FIXED):
                relax(best, other, base + o, PI, PW, PV, o * FIXED + i)
        if not lists:
            for p in range(extra):
                relax(best, other, OFF[g, p] + base, EI, EW, None, p)
        else:
            def more(c, best):
                best = list(best)
                for n in range(CHUNK):
                    relax(best, None, OFF[g, c * CHUNK + n] + base, EI, EW, None, c * CHUNK + n)
                return tuple(best)
            best = lax.fori_loop(0, extra // CHUNK, more, tuple(best))
        return [jnp.minimum(best[k], pltpu.roll(other[k], HALF, 1)) for k in range(rows)]

    def one(t, _):
        @pl.when(t == MEET)
        def _():
            wait_peers()
            for c in shares:
                c.start()

        read = lax.rem(t, 2)
        for g in range(groups):
            for k, value in enumerate(relaxed(read, g)):
                put(X.at[1 - read, k], g, groups, value)
        return 0

    lax.fori_loop(0, SWEEPS - 1, one, 0)

    for c in shares:
        c.wait()
    Q[me] = sum(g * g for g in [gradient(h) for h in range(m)])
    for c in norms:
        c.start()

    per = 8 // m
    seat = lax.rem(me, per)
    outs = []
    for n in range(groups):
        g = lax.rem(me // per + 1 + n, groups)
        for k, value in enumerate(relaxed((SWEEPS - 1) % 2, g)):
            Y[pl.ds(8 * g, 8), k, :] = value
        turns = [(per // 2 + q) % per for q in range(per)]
        ready = []
        for q in turns:
            if n == groups - 1 and q == 0:
                continue
            j = g * per + lax.rem(seat + q, per)
            for h in range(m):
                at = len(outs) + len(ready)
                ready.append(send(Y.at[j * m + h], out_ref.at[me, :, block_lanes[h]], o_s.at[at], o_r.at[at], (mc, j)))
        for c in ready:
            c.start()
        outs += ready
    for h in range(m):
        out_ref[me, :, block_lanes[h]] = Y[me * m + h]
    for c in norms:
        c.wait()
    square = Q[0]
    for i in range(1, A):
        square = square + Q[i]
    scale_root = jnp.sqrt(jnp.sum(square) / (degree * node_count) + eps_value)
    for h in range(m):
        newp_ref[:, block_lanes[h]] = jnp.maximum(
            price_ref[:, block_lanes[h]] + step_size * gradient(h) / scale_root, 0.0)
    for c in outs:
        c.wait()


def store_kernel(out_ref, newp_ref, out_hbm, newp_hbm, sem):
    copies = [pltpu.make_async_copy(out_ref, out_hbm, sem.at[0]), pltpu.make_async_copy(newp_ref, newp_hbm, sem.at[1])]
    for c in copies:
        c.start()
    for c in copies:
        c.wait()


def extras_of(degree):
    return OFFS * (degree - FIXED)


def shards(A, C, prev_dist, source_node, arc_tail, base_cost, arc_price, capacity, path_arcs, demand):
    commodities, span = prev_dist.shape
    degree = arc_tail.shape[0]
    rows = commodities // A
    m = span // LANES
    NB = A * m
    assert NB % 8 == 0 and 8 % m == 0 and A % (8 // m) == 0 and degree >= 2 * FIXED and extras_of(degree) % CHUNK == 0
    f32, i32 = jnp.float32, jnp.int32
    groups = NB // 8
    extras = extras_of(degree)
    pitch = NB + 2 * PAD + (8 if (NB // 8) % 2 == 0 else 0)
    vmem = pl.BlockSpec(memory_space=pltpu.VMEM)
    smem = pl.BlockSpec(memory_space=pltpu.SMEM)
    hbm = pl.BlockSpec(memory_space=pltpu.HBM)
    sems = pltpu.SemaphoreType.DMA
    kept_words = (rows * (NB + 2 * PAD) + 16 * groups * degree + 8 * groups * (OFFS * (2 + 3 * FIXED) + 2 * BUCKETS[-1])) * LANES
    limit = 64_600_000 - 4 * kept_words
    X0, KT, WW, COUNT, CAP, PI, PW, PV, EI, EW, flow, price, cap, OFF, choice = pl.pallas_call(
        functools.partial(gather_kernel, A, C, m),
        out_shape=(pltpu.VMEM((rows, NB + 2 * PAD, LANES), f32), pltpu.VMEM((groups, degree, 8, LANES), i32),
                   pltpu.VMEM((groups, degree, 8, LANES), f32), pltpu.VMEM((groups, OFFS, 8, LANES), i32),
                   pltpu.VMEM((groups, OFFS, 8, LANES), i32),
                   pltpu.VMEM((groups, OFFS * FIXED, 8, LANES), i32),
                   pltpu.VMEM((groups, OFFS * FIXED, 8, LANES), f32),
                   pltpu.VMEM((groups, OFFS * FIXED, 8, LANES), f32),
                   pltpu.VMEM((groups, BUCKETS[-1], 8, LANES), i32), pltpu.VMEM((groups, BUCKETS[-1], 8, LANES), f32),
                   pltpu.VMEM((m * degree, LANES), f32),
                   pltpu.VMEM((degree, span), f32), pltpu.VMEM((degree, span), f32),
                   jax.ShapeDtypeStruct((groups, BUCKETS[-1]), i32), jax.ShapeDtypeStruct((1,), i32)),
        in_specs=[smem] * 2 + [hbm] * 6,
        out_specs=(vmem,) * 13 + (smem,) * 2,
        scratch_shapes=[
            pltpu.VMEM((NB, rows, LANES), f32),
            pltpu.VMEM((A, rows, span), f32),
            pltpu.VMEM((degree, span), i32),
            pltpu.VMEM((degree, span), f32),
            pltpu.VMEM(path_arcs.shape, i32),
            pltpu.VMEM((NB * degree, LANES), i32),
            pltpu.VMEM((NB * degree, LANES), f32),
            pltpu.VMEM((A, m * degree, LANES), f32),
            pltpu.VMEM((A, m * degree, LANES), f32),
        ] + [sems((6,))] + [sems(((A - 1) * m,))] * 2 + [sems((A - 1,))] * 6,
        compiler_params=pltpu.CompilerParams(collective_id=0, has_side_effects=True, vmem_limit_bytes=limit),
    )(source_node, demand, prev_dist.reshape(A, rows, span), arc_tail, base_cost, arc_price, capacity, path_arcs)
    def branch(n, extra):
        return lambda *operands: pl.pallas_call(
            functools.partial(sweep_kernel, A, C, m, extra),
            out_shape=(pltpu.VMEM((A, rows, span), f32), pltpu.VMEM((degree, span), f32)),
            in_specs=[smem] + [vmem] * 13,
            out_specs=(vmem, vmem),
            scratch_shapes=[
                pltpu.VMEM((2, rows, pitch, LANES), f32),
                pltpu.VMEM((NB, rows, LANES), f32),
                pltpu.VMEM((C, m * degree, LANES), f32),
                pltpu.VMEM((A, degree, LANES), f32),
            ] + [sems((C - 1,))] * 2 + [sems((A - 1,))] * 2 + [sems(((A - 1) * m,))] * 2 + ([] if extra in BUCKETS else [
                pltpu.VMEM((groups, extra, 8, LANES), i32),
                pltpu.VMEM((groups, extra, 8, LANES), f32),
                pltpu.SMEM((groups, extra), i32),
            ]),
            compiler_params=pltpu.CompilerParams(collective_id=1 + n, has_side_effects=True, vmem_limit_bytes=24 * 2**20),
        )(*operands)

    out, new_price = lax.switch(choice[0], [branch(n, extra) for n, extra in enumerate(BUCKETS + (extras,))],
                                OFF, X0, KT, WW, COUNT, CAP, PI, PW, PV, EI, EW, flow, price, cap)
    out, new_price = pl.pallas_call(
        store_kernel,
        out_shape=(jax.ShapeDtypeStruct(out.shape, f32), jax.ShapeDtypeStruct(new_price.shape, f32)),
        in_specs=[vmem] * 2,
        out_specs=(hbm, hbm),
        scratch_shapes=[sems((2,))],
        compiler_params=pltpu.CompilerParams(vmem_limit_bytes=24 * 2**20),
    )(out, new_price)
    return (out.reshape(commodities, span), new_price)


def solution(mesh):
    in_specs = (
        P("comm", "arc"),
        P("comm"),
        P(None, "arc"),
        P(None, "arc"),
        P(None, "arc"),
        P(None, "arc"),
        P(("comm", "arc"), None),
        P(("comm", "arc")),
    )
    out_specs = (P("comm", "arc"), P(None, "arc"))
    body = functools.partial(shards, mesh.shape["arc"], mesh.shape["comm"])
    return jax.shard_map(body, mesh=mesh, in_specs=in_specs, out_specs=out_specs, check_vma=False)
```
